512 devices in a mesh: dp: 32 (over z, core), tp: 16 (over x, y).
Axes of the slice: x: 4, y: 4, z: 16, core: 2. Of those that a mesh axis runs over, the one named last changes fastest.
Arguments:
- partials: bfloat16 [16, 5120, 7680], P('tp', 'dp'), may hold values from -1.5 to 1.5
- layer_input: bfloat16 [7680, 1280], P(('dp', 'tp')), may hold values from -6 to 6
- ln_gain: float32 [1280], replicated, may hold values from 0.25 to 1.75
- ln_bias: float32 [1280], replicated, may hold values from -3 to 3
- fc1_weight: bfloat16 [1280, 5120], P(None, 'tp'), may hold values from -0.15625 to 0.15625
- fc1_bias: float32 [5120], P('tp'), may hold values from -3 to 3
- fc2_weight: bfloat16 [1280, 5120], P(None, 'tp'), may hold values from -0.078125 to 0.078125
- row_rank: int32 [5120, 1], P('dp'), may hold values from 0 to 15; in each aligned block of 160 rows (0 to 159, 160 to 319, ...) at most 15 rows name the same one
Outputs:
- early_grads: bfloat16 [7680, 6400], P(('dp', 'tp'))
- fc1_grad: bfloat16 [1280, 5120], P('dp', 'tp')
- fc2_grad: bfloat16 [1280, 5120], P('dp', 'tp')
The draws below stay inside these ranges and needn't reach their ends.
Inputs may be any that keep to these rules, and one draw needn't show every extreme that they name: `row_rank`: in each aligned block of 160 rows (one data replica) no rank is named by more than 15 rows, a bound that some block reaches.
All inputs are finite; a program needn't handle non-finite values.
Results may differ from the reference program's by a relative error of at most 0.029.
Values may be sent and summed in bfloat16 or wider, within the bound.
No kernel may reach another device: no remote copies, remote signals or barrier semaphores. Data moves between devices by JAX's collectives and lax.ppermute only.
A program may use at most 64 MiB of HBM per device.

```python
import math
import jax
import jax.numpy as jnp
import numpy as np
from jax import lax

D = 1280
HID = 5120
VIS = 7680
ROWS = 160
MOST = 15
TOTAL_ROWS = 5120
SLOTS = 7680
N_DP = 32
N_TP = 16


def level_of(stream_key, shape, shards, smallest, high):
    loudness, own = 1.0, jax.random.fold_in(stream_key, 6)
    for axis_at, parts in shards:
        steps = jnp.exp(jax.random.uniform(jax.random.fold_in(own, axis_at), (parts,), jnp.float32, smallest / len(shards), high / len(shards)))
        loudness = loudness * jnp.repeat(steps, shape[axis_at] // parts).reshape([-1 if axis == axis_at else 1 for axis in range(len(shape))])
    return loudness


def routed_block(own_key, own, number, rows, amount, top, most, lean):
    ranking = jax.random.permutation(own_key, amount)
    packed, usual = shares(amount, rows * top, most, lean, True), shares(amount, rows * top, most, lean, False)
    places = jnp.arange(amount)

    def named(tallies, rotation):
        used = int((tallies > 0).sum())
        fixed = max(1, used // 4)
        moved = fixed + (places - fixed + rotation * (used - fixed)) % max(1, amount - fixed)
        return jnp.zeros((amount,), jnp.int32).at[ranking[jnp.where(places < fixed, places, moved)]].set(jnp.asarray(tallies, jnp.int32))

    tallies = jnp.where(number % 4 == 0, named(packed, number // 4), named(usual, number - number // 4 - 1))
    mixed = jax.random.permutation(jax.random.fold_in(own, 3), amount)
    giver, sink = mixed[0:amount // 2 * 2:2], mixed[1:amount // 2 * 2:2]
    room = jnp.minimum(tallies[giver] - 1, most - tallies[sink]) // 2
    room = jnp.where((giver == ranking[0]) | (sink == ranking[0]) | (tallies[sink] == 0), 0, jnp.maximum(room, 0))
    moved = jax.random.randint(jax.random.fold_in(own, 4), (amount // 2,), 0, 1 << 20) % (room + 1)
    tallies = tallies.at[giver].add(-moved).at[sink].add(moved)
    members = jnp.searchsorted(jnp.cumsum(tallies), jnp.arange(rows * top), side="right").astype(jnp.int32)
    grid = members.reshape(top, rows).T
    grid = grid[jax.random.permutation(jax.random.fold_in(own, 1), rows)]
    rotation = jax.random.randint(jax.random.fold_in(own, 2), (rows, 1), 0, top)
    return jnp.take_along_axis(grid, (jnp.arange(top)[None, :] + rotation) % top, axis=1)


def shares(amount, total, most, skew, full):
    weights = [(1 << 20) // math.isqrt(standing ** skew) + 1 for standing in range(1, amount + 1)]
    largest = most if full else min(most, max(-(-total // amount), total * weights[0] // sum(weights)))
    least = 1 if total - largest >= amount - 1 else 0
    given, spare = [largest] + [least] * (amount - 1), total - largest - least * (amount - 1)
    while spare > 0:
        candidates = [i for i in range(1, amount) if given[i] < largest] or [i for i in range(1, amount) if given[i] < most]
        pool, left = sum([weights[i] for i in candidates]), spare
        for i in candidates:
            more = min(most - given[i], max(1, left * weights[i] // pool), spare)
            given[i] = given[i] + more
            spare = spare - more
    return np.array(given)


def gaussian(own_key, extent, scale, most, shards=(), kind=jnp.bfloat16):
    gain = level_of(own_key, extent, shards, -0.22, 0.18) if shards else 1.0
    drawn = jax.random.normal(own_key, extent, jnp.float32) * scale * gain
    return jnp.minimum(jnp.maximum(drawn, -most), most).astype(kind)


def setup_inputs(seed: int = 0) -> dict:
    key_of = jax.random.split(jax.random.key(seed), 9)
    partials = gaussian(key_of[0], (N_TP, TOTAL_ROWS, VIS), 0.25, 1.5, ((0, 16), (1, 32)))
    layer_input = gaussian(key_of[1], (SLOTS, D), 1.0, 6.0, ((0, 512),))
    ln_gain = jnp.clip(1.0 + 0.15 * jax.random.normal(key_of[2], (D,), jnp.float32), 0.25, 1.75)
    ln_bias = gaussian(key_of[3], (D,), 0.5, 3.0, (), jnp.float32)
    fc1_weight = gaussian(key_of[4], (D, HID), D ** -0.5, 0.15625, ((1, 16),))
    fc1_bias = gaussian(key_of[5], (HID,), 0.5, 3.0, ((0, 16),), jnp.float32)
    fc2_weight = gaussian(key_of[6], (D, HID), HID ** -0.5, 0.078125, ((1, 16),))
    row_rank_keys = jax.random.split(jax.random.fold_in(key_of[7], 1), TOTAL_ROWS // ROWS)
    row_rank_turns = jax.random.permutation(jax.random.fold_in(key_of[7], 3), TOTAL_ROWS // ROWS)
    row_rank = jax.vmap(lambda own, number: routed_block(jax.random.fold_in(key_of[7], 2), own, number, ROWS, N_TP, 1, MOST, 2))(row_rank_keys, row_rank_turns).reshape((TOTAL_ROWS, 1))
    return dict(partials=partials, layer_input=layer_input, ln_gain=ln_gain, ln_bias=ln_bias, fc1_weight=fc1_weight, fc1_bias=fc1_bias, fc2_weight=fc2_weight, row_rank=row_rank)


def gelu_parts(preact):
    normal_cdf = 0.5 * (1.0 + lax.erf(preact * 0.7071067811865476))
    density = jnp.exp(-0.5 * preact * preact) * 0.3989422804014327
    return (preact * normal_cdf, normal_cdf + preact * density)

def slot_matrix(rank_ids, groups, slot_count):
    columns = jnp.arange(groups, dtype=jnp.int32)
    onehot = (rank_ids[:, None] == columns[None, :]).astype(jnp.int32)
    position = jnp.cumsum(onehot, axis=0) - 1
    own_position = lax.optimization_barrier(jnp.sum(position * onehot, axis=1))
    slot_ids = rank_ids * slot_count + own_position
    targets = jnp.arange(groups * slot_count, dtype=jnp.int32)
    return (targets[:, None] == slot_ids[None, :]).astype(jnp.bfloat16)

def normalize(layer_rows, ln_gain, ln_bias):
    values = layer_rows.astype(jnp.float32)
    row_mean = lax.optimization_barrier(jnp.mean(values, axis=1, keepdims=True))
    centered = values - row_mean
    row_var = lax.optimization_barrier(jnp.mean(centered * centered, axis=1, keepdims=True))
    return (centered / jnp.sqrt(row_var + 1e-05) * ln_gain + ln_bias).astype(jnp.bfloat16)

def reference(partials, layer_input, ln_gain, ln_bias, fc1_weight, fc1_bias, fc2_weight, row_rank):
    factor = float(N_DP * ROWS) ** (-0.5)

    def replica_step(carry, replica):
        first_sum, second_sum = carry
        replica_parts = lax.dynamic_slice_in_dim(partials, replica * ROWS, ROWS, 1)
        summed = lax.optimization_barrier(jnp.sum(replica_parts.astype(jnp.float32), axis=0)).astype(jnp.bfloat16)
        rank_ids = lax.dynamic_slice_in_dim(row_rank[:, 0], replica * ROWS, ROWS, 0).astype(jnp.int32)
        table = slot_matrix(rank_ids, N_TP, MOST)
        placed = jnp.dot(table, summed, preferred_element_type=jnp.float32).astype(jnp.bfloat16)
        layer_rows = lax.dynamic_slice_in_dim(layer_input, replica * N_TP * MOST, N_TP * MOST, 0)
        normed = normalize(layer_rows, ln_gain, ln_bias)
        upstream = placed[:, :D]
        preact = jnp.dot(normed, fc1_weight, preferred_element_type=jnp.float32) + fc1_bias
        activated, derivative = gelu_parts(preact)
        hidden = activated.astype(jnp.bfloat16)
        hidden_grad = jnp.dot(upstream, fc2_weight, preferred_element_type=jnp.float32)
        preact_grad = (hidden_grad * derivative).astype(jnp.bfloat16)
        grad_first = (jnp.dot(normed.T, preact_grad, preferred_element_type=jnp.float32) * factor).astype(jnp.bfloat16)
        grad_second = (jnp.dot(upstream.T, hidden, preferred_element_type=jnp.float32) * factor).astype(jnp.bfloat16)
        carry = (first_sum + grad_first.astype(jnp.float32), second_sum + grad_second.astype(jnp.float32))
        return (carry, placed[:, D:])
    start = (jnp.zeros((D, HID), jnp.float32), jnp.zeros((D, HID), jnp.float32))
    (first_sum, second_sum), early = lax.scan(replica_step, start, jnp.arange(N_DP, dtype=jnp.int32))
    early_grads = early.reshape(N_DP * N_TP * MOST, VIS - D)
    return (early_grads, first_sum.astype(jnp.bfloat16), second_sum.astype(jnp.bfloat16))
```

```python
import functools

import jax
import jax.numpy as jnp
from jax import lax
from jax.experimental import pallas as pl
from jax.experimental.pallas import tpu as pltpu
from jax.sharding import PartitionSpec as P

SUB, LANE = 8, 128
SLOT_PAD = 16


def tile_places(rows, width, parts):
    across = width // LANE
    total = (rows // SUB) * across
    whole = total // parts
    places = []
    for t in range(total):
        r, c = divmod(t, across)
        if t < whole * parts:
            places.append((*divmod(t, whole), 0, SUB, r * SUB, c * LANE))
        else:
            half = SUB // 2
            for h in range(2):
                part = 2 * (t - whole * parts) + h
                places.append((part, whole, 0, half, r * SUB + h * half, c * LANE))
    return whole + 1, places


def cut_kernel(places, x_ref, out_ref):
    last = out_ref.shape[1] - 1
    for part in range(out_ref.shape[0]):
        out_ref[part, last] = jnp.zeros(out_ref.shape[2:], out_ref.dtype)
    for part, i, at, size, r, c in places:
        out_ref[part, i, at : at + size, :] = x_ref[r : r + size, c : c + LANE]


def cut_tiles(x, width, parts):
    rows = x.shape[0]
    depth, places = tile_places(rows, width, parts)
    return pl.pallas_call(
        functools.partial(cut_kernel, places),
        grid=(1,),
        in_specs=[pl.BlockSpec((rows, width), lambda i: (0, 0))],
        out_specs=pl.BlockSpec((parts, depth, SUB, LANE), lambda i: (0, 0, 0, 0)),
        out_shape=jax.ShapeDtypeStruct((parts, depth, SUB, LANE), x.dtype),
        name="cut_tiles",
    )(x)


def grads_kernel(places, factor, tiles_ref, table_ref, normed_ref, hidden_ref, deriv_ref, weight_ref, out_ref, rows_ref, up_ref, pg_ref):
    for part, i, at, size, r, c in places:
        rows_ref[r : r + size, c : c + LANE] = tiles_ref[part, i, at : at + size, :]
    up_ref[...] = jnp.dot(table_ref[...], rows_ref[...], preferred_element_type=jnp.float32).astype(jnp.bfloat16)
    hidden_grad = lax.dot_general(
        up_ref[...], weight_ref[...], (((1,), (1,)), ((), ())), preferred_element_type=jnp.float32
    )
    units = hidden_grad.shape[1]
    pg_ref[...] = jnp.zeros_like(pg_ref)
    pg_ref[:, :units] = (hidden_grad * deriv_ref[...]).astype(jnp.bfloat16)
    cores, near, far, block, _ = out_ref.shape
    wide = pg_ref.shape[1]
    keep = wide - LANE
    step = 5 * LANE
    for at in range(0, normed_ref.shape[1], step):
        dims = (((0,), (0,)), ((), ()))
        first = lax.dot_general(normed_ref[:, at : at + step], pg_ref[...], dims, preferred_element_type=jnp.float32)
        second = lax.dot_general(up_ref[:, at : at + step], hidden_ref[...], dims, preferred_element_type=jnp.float32)
        for b in range(0, step, block):
            k = (at + b) // block
            z, core = divmod(k, cores)
            m, p = divmod(z, near)
            one, two = first[b : b + block] * factor, second[b : b + block] * factor
            out_ref[core, p, m, :, :keep] = one[:, :keep].astype(jnp.bfloat16)
            out_ref[core, p, m, :, keep:wide] = (one[:, keep:] + two[:, :LANE]).astype(jnp.bfloat16)
            out_ref[core, p, m, :, wide:] = two[:, LANE:].astype(jnp.bfloat16)


def grad_terms(tiles, table, normed, hidden, deriv, weight_t, factor, shape):
    slots, width = normed.shape
    rows = table.shape[1]
    _, places = tile_places(rows, width, tiles.shape[0])
    return pl.pallas_call(
        functools.partial(grads_kernel, places, factor),
        out_shape=jax.ShapeDtypeStruct(shape, jnp.bfloat16),
        scratch_shapes=[
            pltpu.VMEM((rows, width), jnp.bfloat16),
            pltpu.VMEM((slots, width), jnp.bfloat16),
            pltpu.VMEM((slots, hidden.shape[1]), jnp.bfloat16),
        ],
        name="grad_terms",
    )(tiles, table, normed, hidden, deriv, weight_t)


def exchange(blocks, axis, groups=None):
    return lax.all_to_all(blocks, axis, 0, 0, tiled=True, axis_index_groups=groups)


def to_all(shard, axis):
    return exchange(jnp.broadcast_to(shard, (lax.axis_size(axis), *shard.shape)), axis)


def total(arrived):
    return arrived.astype(jnp.float32).sum(axis=0).astype(jnp.bfloat16)


def gelu_parts(preact):
    normal_cdf = 0.5 * (1.0 + lax.erf(preact * 0.7071067811865476))
    density = jnp.exp(-0.5 * preact * preact) * 0.3989422804014327
    return (preact * normal_cdf, normal_cdf + preact * density)


def slot_matrix(rank_ids, groups):
    columns = jnp.arange(groups, dtype=jnp.int32)
    onehot = (rank_ids[:, None] == columns[None, :]).astype(jnp.int32)
    position = jnp.cumsum(onehot, axis=0) - 1
    own_position = jnp.sum(position * onehot, axis=1)
    slot_ids = rank_ids * SLOT_PAD + own_position
    targets = jnp.arange(groups * SLOT_PAD, dtype=jnp.int32)
    return (targets[:, None] == slot_ids[None, :]).astype(jnp.bfloat16)


def normalize(layer_rows, ln_gain, ln_bias):
    values = layer_rows.astype(jnp.float32)
    row_mean = jnp.mean(values, axis=1, keepdims=True)
    centered = values - row_mean
    row_var = jnp.mean(centered * centered, axis=1, keepdims=True)
    return (centered / jnp.sqrt(row_var + 1e-05) * ln_gain + ln_bias).astype(jnp.bfloat16)


def dp_groups(replicas):
    cores, near = 2, 4
    depth = replicas // cores
    far = depth // near
    pairs = [[cores * z + c for c in range(cores)] for z in range(depth)]
    close = []
    for g in range(far):
        close.append([cores * (near * g + p) for p in range(near)])
    for g in range(far):
        zs = [(near * (g + 1) + p) % depth if p < near // 2 else near * g + p for p in range(near)]
        close.append([cores * z + 1 for z in zs])
    strided = [[cores * (near * m + p) + c for m in range(far)] for p in range(near) for c in range(cores)]
    return cores, near, far, pairs, close, strided


def shards(partials, layer_input, ln_gain, ln_bias, fc1_weight, fc1_bias, fc2_weight, row_rank):
    groups = lax.axis_size("tp")
    replicas = lax.axis_size("dp")
    local_part = partials[0]
    row_count = local_part.shape[0]
    slot_count, width = layer_input.shape
    units = fc1_weight.shape[1]
    cores, near, far, pairs, close, strided = dp_groups(replicas)
    block = width // replicas

    outgoing = cut_tiles(local_part, width, groups)
    own_tiles = total(exchange(outgoing, "tp"))
    tiles = to_all(own_tiles, "tp")

    table = slot_matrix(row_rank[:, 0], groups)
    normed = normalize(layer_input, ln_gain, ln_bias)
    normed = jnp.pad(normed, ((0, SLOT_PAD - slot_count), (0, 0)))
    normed_all = to_all(normed, "tp").reshape(groups * SLOT_PAD, width)
    preact = jnp.dot(normed_all, fc1_weight, preferred_element_type=jnp.float32) + fc1_bias
    activated, derivative = gelu_parts(preact)
    hidden = jnp.pad(activated.astype(jnp.bfloat16), ((0, 0), (-units % LANE, 0)))

    routed = jnp.dot(table, local_part[:, width:], preferred_element_type=jnp.float32).astype(jnp.bfloat16)
    incoming = exchange(routed.reshape(groups, SLOT_PAD, routed.shape[1]), "tp")

    factor = float(replicas * row_count) ** (-0.5)
    terms = grad_terms(
        tiles, table, normed_all, hidden, derivative, fc2_weight.T, factor,
        (cores, near, far, block, 2 * units),
    )
    both = total(exchange(terms, "dp", pairs))
    both = total(exchange(both, "dp", close))
    both = total(exchange(both, "dp", strided))
    placed = total(incoming)[:slot_count]
    return (placed, both[:, :units], both[:, units:])


def solution(mesh):
    return jax.shard_map(
        shards,
        mesh=mesh,
        in_specs=(
            P("tp", "dp", None),
            P(("dp", "tp"), None),
            P(),
            P(),
            P(None, "tp"),
            P("tp"),
            P(None, "tp"),
            P("dp", None),
        ),
        out_specs=(P(("dp", "tp"), None), P("dp", "tp"), P("dp", "tp")),
        check_vma=False,
    )
```

```python
import functools

import jax
import jax.numpy as jnp
from jax import lax
from jax.experimental import pallas as pl
from jax.experimental.pallas import tpu as pltpu
from jax.sharding import PartitionSpec as P

SUB, LANE = 8, 128
SLOT_PAD = 16


def tile_places(rows, width, parts):
    across = width // LANE
    total = (rows // SUB) * across
    whole = total // parts
    places = []
    for t in range(total):
        r, c = divmod(t, across)
        if t < whole * parts:
            places.append((*divmod(t, whole), 0, SUB, r * SUB, c * LANE))
        else:
            half = SUB // 2
            for h in range(2):
                part = 2 * (t - whole * parts) + h
                places.append((part, whole, 0, half, r * SUB + h * half, c * LANE))
    return whole + 1, places


def cut_kernel(places, x_ref, layer_ref, out_ref):
    parts, depth = out_ref.shape[:2]
    slot_count, width = layer_ref.shape
    across = width // LANE
    head = depth - (SLOT_PAD // SUB) * across
    for part, i, at, size, r, c in places:
        out_ref[part, i, at : at + size, :] = x_ref[r : r + size, c : c + LANE]
        if size < SUB:
            out_ref[part, i, size:, :] = jnp.zeros((SUB - size, LANE), out_ref.dtype)
    for at in range(0, SLOT_PAD, SUB):
        size = min(SUB, slot_count - at)
        for c in range(across):
            tile = layer_ref[at : at + size, c * LANE : (c + 1) * LANE]
            for part in range(parts):
                out_ref[part, head + (at // SUB) * across + c, :size, :] = tile
                if size < SUB:
                    out_ref[part, head + (at // SUB) * across + c, size:, :] = jnp.zeros((SUB - size, LANE), tile.dtype)


def cut_tiles(x, layer, parts):
    rows, width = x.shape[0], layer.shape[1]
    depth, places = tile_places(rows, width, parts)
    depth += (SLOT_PAD // SUB) * (width // LANE)
    return pl.pallas_call(
        functools.partial(cut_kernel, places),
        grid=(1,),
        in_specs=[pl.BlockSpec((rows, width), lambda i: (0, 0)), pl.BlockSpec(layer.shape, lambda i: (0, 0))],
        out_specs=pl.BlockSpec((parts, depth, SUB, LANE), lambda i: (0, 0, 0, 0)),
        out_shape=jax.ShapeDtypeStruct((parts, depth, SUB, LANE), x.dtype),
        name="cut_tiles",
    )(x, layer)


def gelu_parts(preact):
    normal_cdf = 0.5 * (1.0 + lax.erf(preact * 0.7071067811865476))
    density = jnp.exp(-0.5 * preact * preact) * 0.3989422804014327
    return (preact * normal_cdf, normal_cdf + preact * density)


def hidden_kernel(head, tiles_ref, gain_ref, bias_ref, weight_ref, fc1_bias_ref, normed_ref, hidden_ref, deriv_ref):
    parts = tiles_ref.shape[0]
    slots, width = normed_ref.shape
    across = width // LANE
    per_part = slots // parts
    for part in range(parts):
        for at in range(0, per_part, SUB):
            for c in range(across):
                normed_ref[part * per_part + at : part * per_part + at + SUB, c * LANE : (c + 1) * LANE] = tiles_ref[
                    part, head + (at // SUB) * across + c
                ]
    values = normed_ref[...].astype(jnp.float32)
    centered = values - jnp.mean(values, axis=1, keepdims=True)
    row_var = jnp.mean(centered * centered, axis=1, keepdims=True)
    normed = (centered / jnp.sqrt(row_var + 1e-05) * gain_ref[...] + bias_ref[...]).astype(jnp.bfloat16)
    normed_ref[...] = normed
    preact = lax.dot_general(normed, weight_ref[...], (((1,), (1,)), ((), ())), preferred_element_type=jnp.float32)
    activated, derivative = gelu_parts(preact + fc1_bias_ref[...])
    gap = hidden_ref.shape[1] - activated.shape[1]
    hidden_ref[...] = jnp.zeros_like(hidden_ref)
    hidden_ref[:, gap:] = activated.astype(jnp.bfloat16)
    deriv_ref[...] = derivative


def hidden_parts(tiles, head, gain, bias, weight_t, fc1_bias):
    units, width = weight_t.shape
    slots = tiles.shape[0] * SLOT_PAD
    wide = -(-units // LANE) * LANE
    return pl.pallas_call(
        functools.partial(hidden_kernel, head),
        out_shape=(
            jax.ShapeDtypeStruct((slots, width), jnp.bfloat16),
            jax.ShapeDtypeStruct((slots, wide), jnp.bfloat16),
            jax.ShapeDtypeStruct((slots, units), jnp.float32),
        ),
        name="hidden_parts",
    )(tiles, gain[None], bias[None], weight_t, fc1_bias[None])


def grads_kernel(places, factor, tiles_ref, table_ref, normed_ref, hidden_ref, deriv_ref, weight_ref, out_ref, rows_ref, up_ref, pg_ref):
    for part, i, at, size, r, c in places:
        rows_ref[r : r + size, c : c + LANE] = tiles_ref[part, i, at : at + size, :]
    up_ref[...] = jnp.dot(table_ref[...], rows_ref[...], preferred_element_type=jnp.float32).astype(jnp.bfloat16)
    hidden_grad = lax.dot_general(
        up_ref[...], weight_ref[...], (((1,), (1,)), ((), ())), preferred_element_type=jnp.float32
    )
    units = hidden_grad.shape[1]
    pg_ref[...] = jnp.zeros_like(pg_ref)
    pg_ref[:, :units] = (hidden_grad * deriv_ref[...]).astype(jnp.bfloat16)
    cores, near, far, block, _ = out_ref.shape
    wide = pg_ref.shape[1]
    keep = wide - LANE
    step = 5 * LANE
    for at in range(0, normed_ref.shape[1], step):
        dims = (((0,), (0,)), ((), ()))
        first = lax.dot_general(normed_ref[:, at : at + step], pg_ref[...], dims, preferred_element_type=jnp.float32)
        second = lax.dot_general(up_ref[:, at : at + step], hidden_ref[...], dims, preferred_element_type=jnp.float32)
        for b in range(0, step, block):
            k = (at + b) // block
            z, core = divmod(k, cores)
            m, p = divmod(z, near)
            one, two = first[b : b + block] * factor, second[b : b + block] * factor
            out_ref[core, p, m, :, :keep] = one[:, :keep].astype(jnp.bfloat16)
            out_ref[core, p, m, :, keep:wide] = (one[:, keep:] + two[:, :LANE]).astype(jnp.bfloat16)
            out_ref[core, p, m, :, wide:] = two[:, LANE:].astype(jnp.bfloat16)


def grad_terms(tiles, table, normed, hidden, deriv, weight_t, factor, shape):
    slots, width = normed.shape
    rows = table.shape[1]
    _, places = tile_places(rows, width, tiles.shape[0])
    return pl.pallas_call(
        functools.partial(grads_kernel, places, factor),
        out_shape=jax.ShapeDtypeStruct(shape, jnp.bfloat16),
        scratch_shapes=[
            pltpu.VMEM((rows, width), jnp.bfloat16),
            pltpu.VMEM((slots, width), jnp.bfloat16),
            pltpu.VMEM((slots, hidden.shape[1]), jnp.bfloat16),
        ],
        name="grad_terms",
    )(tiles, table, normed, hidden, deriv, weight_t)


def exchange(blocks, axis, groups=None):
    return lax.all_to_all(blocks, axis, 0, 0, tiled=True, axis_index_groups=groups)


def to_all(shard, axis):
    return exchange(jnp.broadcast_to(shard, (lax.axis_size(axis), *shard.shape)), axis)


def total(arrived):
    return arrived.astype(jnp.float32).sum(axis=0).astype(jnp.bfloat16)


def slot_positions(rank_ids, groups):
    columns = jnp.arange(groups, dtype=jnp.int32)
    onehot = (rank_ids[:, None] == columns[None, :]).astype(jnp.int32)
    position = jnp.cumsum(onehot, axis=0) - 1
    return jnp.sum(position * onehot, axis=1)


def slot_table(slot_ids, first, count):
    targets = first + jnp.arange(count, dtype=jnp.int32)
    return (targets[:, None] == slot_ids[None, :]).astype(jnp.bfloat16)


def plane_rounds(replicas, side):
    rounds = []
    for turn in range(2):
        perms = []
        for d in range(1, side):
            pairs = []
            for k in range(replicas):
                for x in range(side):
                    for y in range(side):
                        along_x = (k % 2 == 0) == (turn == 0)
                        to = ((x + d) % side, y) if along_x else (x, (y + d) % side)
                        pairs.append(((k * side + x) * side + y, (k * side + to[0]) * side + to[1]))
            perms.append(pairs)
        rounds.append(perms)
    return rounds


def route_early(part, rank_ids, positions, replicas, groups):
    side = int(groups**0.5)
    rounds = plane_rounds(replicas, side)
    me = lax.axis_index("tp")
    dx = (rank_ids // side - me // side) % side
    dy = (rank_ids % side - me % side) % side
    x_first = lax.axis_index("dp") % 2 == 0
    first, second = jnp.where(x_first, dx, dy), jnp.where(x_first, dy, dx)
    slot_ids = (first * side + second) * SLOT_PAD + positions
    span = side * SLOT_PAD
    blocks = [
        jnp.dot(slot_table(slot_ids, d * span, span), part, preferred_element_type=jnp.float32).astype(jnp.bfloat16)
        for d in range(side)
    ]
    moved = [lax.ppermute(blocks[d], ("dp", "tp"), rounds[0][d - 1]) for d in range(1, side)]
    summed = sum((b.astype(jnp.float32) for b in moved), blocks[0].astype(jnp.float32)).astype(jnp.bfloat16)
    pieces = [summed[d * SLOT_PAD : (d + 1) * SLOT_PAD] for d in range(side)]
    moved = [lax.ppermute(pieces[d], ("dp", "tp"), rounds[1][d - 1]) for d in range(1, side)]
    return sum((b.astype(jnp.float32) for b in moved), pieces[0].astype(jnp.float32)).astype(jnp.bfloat16)


def dp_groups(replicas):
    cores, near = 2, 4
    depth = replicas // cores
    far = depth // near
    pairs = [[cores * z + c for c in range(cores)] for z in range(depth)]
    close = []
    for g in range(far):
        close.append([cores * (near * g + p) for p in range(near)])
    for g in range(far):
        zs = [(near * (g + 1) + p) % depth if p < near // 2 else near * g + p for p in range(near)]
        close.append([cores * z + 1 for z in zs])
    strided = [[cores * (near * m + p) + c for m in range(far)] for p in range(near) for c in range(cores)]
    return cores, near, far, pairs, close, strided


def shards(partials, layer_input, ln_gain, ln_bias, fc1_weight, fc1_bias, fc2_weight, row_rank):
    groups = lax.axis_size("tp")
    replicas = lax.axis_size("dp")
    local_part = partials[0]
    row_count = local_part.shape[0]
    slot_count, width = layer_input.shape
    units = fc1_weight.shape[1]
    cores, near, far, pairs, close, strided = dp_groups(replicas)
    block = width // replicas

    arrived = exchange(cut_tiles(local_part, layer_input, groups), "tp")
    head = arrived.shape[1] - (SLOT_PAD // SUB) * (width // LANE)
    tiles = to_all(total(arrived[:, :head]), "tp")

    rank_ids = row_rank[:, 0]
    positions = slot_positions(rank_ids, groups)
    table = slot_table(rank_ids * SLOT_PAD + positions, 0, groups * SLOT_PAD)
    normed_all, hidden, derivative = hidden_parts(arrived, head, ln_gain, ln_bias, fc1_weight.T, fc1_bias)
    placed = route_early(local_part[:, width:], rank_ids, positions, replicas, groups)[:slot_count]

    factor = float(replicas * row_count) ** (-0.5)
    terms = grad_terms(
        tiles, table, normed_all, hidden, derivative, fc2_weight.T, factor,
        (cores, near, far, block, 2 * units),
    )
    both = total(exchange(terms, "dp", pairs))
    both = total(exchange(both, "dp", close))
    both = total(exchange(both, "dp", strided))
    return (placed, both[:, :units], both[:, units:])


def solution(mesh):
    return jax.shard_map(
        shards,
        mesh=mesh,
        in_specs=(
            P("tp", "dp", None),
            P(("dp", "tp"), None),
            P(),
            P(),
            P(None, "tp"),
            P("tp"),
            P(None, "tp"),
            P("dp", None),
        ),
        out_specs=(P(("dp", "tp"), None), P("dp", "tp"), P("dp", "tp")),
        check_vma=False,
    )
```

```python
import functools

import jax
import jax.numpy as jnp
from jax import lax
from jax.experimental import pallas as pl
from jax.experimental.pallas import tpu as pltpu
from jax.sharding import PartitionSpec as P


SUB, LANE = 8, 128
SLOT_PAD = 16


def tile_places(rows, width, parts):
    across = width // LANE
    total = (rows // SUB) * across
    whole = total // parts
    places = []
    for t in range(total):
        r, c = divmod(t, across)
        if t < whole * parts:
            places.append((*divmod(t, whole), 0, SUB, r * SUB, c * LANE))
        else:
            half = SUB // 2
            for h in range(2):
                part = 2 * (t - whole * parts) + h
                places.append((part, whole, 0, half, r * SUB + h * half, c * LANE))
    return whole + 1, places


def cut_kernel(places, x_ref, layer_ref, out_ref):
    parts, depth = out_ref.shape[:2]
    slot_count, width = layer_ref.shape
    across = width // LANE
    head = depth - (SLOT_PAD // SUB) * across
    for part, i, at, size, r, c in places:
        out_ref[part, i, at : at + size, :] = x_ref[r : r + size, c : c + LANE]
        if size < SUB:
            out_ref[part, i, size:, :] = jnp.zeros((SUB - size, LANE), out_ref.dtype)
    for at in range(0, SLOT_PAD, SUB):
        size = min(SUB, slot_count - at)
        for c in range(across):
            tile = layer_ref[at : at + size, c * LANE : (c + 1) * LANE]
            for part in range(parts):
                out_ref[part, head + (at // SUB) * across + c, :size, :] = tile
                if size < SUB:
                    out_ref[part, head + (at // SUB) * across + c, size:, :] = jnp.zeros((SUB - size, LANE), tile.dtype)


def cut_tiles(x, layer, parts):
    rows, width = x.shape[0], layer.shape[1]
    depth, places = tile_places(rows, width, parts)
    depth += (SLOT_PAD // SUB) * (width // LANE)
    return pl.pallas_call(
        functools.partial(cut_kernel, places),
        grid=(1,),
        in_specs=[pl.BlockSpec((rows, width), lambda i: (0, 0)), pl.BlockSpec(layer.shape, lambda i: (0, 0))],
        out_specs=pl.BlockSpec((parts, depth, SUB, LANE), lambda i: (0, 0, 0, 0)),
        out_shape=jax.ShapeDtypeStruct((parts, depth, SUB, LANE), x.dtype),
        name="cut_tiles",
    )(x, layer)


def gelu_parts(preact):
    normal_cdf = 0.5 * (1.0 + lax.erf(preact * 0.7071067811865476))
    density = jnp.exp(-0.5 * preact * preact) * 0.3989422804014327
    return (preact * normal_cdf, normal_cdf + preact * density)


def hidden_kernel(head, tiles_ref, gain_ref, bias_ref, weight_ref, fc1_bias_ref, normed_ref, hidden_ref, deriv_ref):
    parts = tiles_ref.shape[0]
    slots, width = normed_ref.shape
    across = width // LANE
    per_part = slots // parts
    for part in range(parts):
        for at in range(0, per_part, SUB):
            for c in range(across):
                normed_ref[part * per_part + at : part * per_part + at + SUB, c * LANE : (c + 1) * LANE] = tiles_ref[
                    part, head + (at // SUB) * across + c
                ]
    values = normed_ref[...].astype(jnp.float32)
    centered = values - jnp.mean(values, axis=1, keepdims=True)
    row_var = jnp.mean(centered * centered, axis=1, keepdims=True)
    normed = (centered / jnp.sqrt(row_var + 1e-05) * gain_ref[...][None] + bias_ref[...][None]).astype(jnp.bfloat16)
    normed_ref[...] = normed
    preact = lax.dot_general(normed, weight_ref[...], (((1,), (1,)), ((), ())), preferred_element_type=jnp.float32)
    activated, derivative = gelu_parts(preact + fc1_bias_ref[...][None])
    gap = hidden_ref.shape[1] - activated.shape[1]
    hidden_ref[...] = jnp.zeros_like(hidden_ref)
    hidden_ref[:, gap:] = activated.astype(jnp.bfloat16)
    deriv_ref[...] = derivative


def hidden_parts(tiles, head, gain, bias, weight_t, fc1_bias):
    units, width = weight_t.shape
    slots = tiles.shape[0] * SLOT_PAD
    wide = -(-units // LANE) * LANE
    return pl.pallas_call(
        functools.partial(hidden_kernel, head),
        out_shape=(
            jax.ShapeDtypeStruct((slots, width), jnp.bfloat16),
            jax.ShapeDtypeStruct((slots, wide), jnp.bfloat16),
            jax.ShapeDtypeStruct((slots, units), jnp.float32),
        ),
        name="hidden_parts",
    )(tiles, gain, bias, weight_t, fc1_bias)


def grads_kernel(places, factor, tiles_ref, table_ref, normed_ref, hidden_ref, deriv_ref, weight_ref, mine_ref, theirs_ref, rows_ref, up_ref, pg_ref):
    for part, i, at, size, r, c in places:
        rows_ref[r : r + size, c : c + LANE] = tiles_ref[part, i, at : at + size, :]
    up_ref[...] = jnp.dot(table_ref[...], rows_ref[...], preferred_element_type=jnp.float32).astype(jnp.bfloat16)
    hidden_grad = lax.dot_general(
        up_ref[...], weight_ref[...], (((1,), (1,)), ((), ())), preferred_element_type=jnp.float32
    )
    units = hidden_grad.shape[1]
    pg_ref[...] = jnp.zeros_like(pg_ref)
    pg_ref[:, :units] = (hidden_grad * deriv_ref[...]).astype(jnp.bfloat16)
    near, _, block, _ = mine_ref.shape
    wide = pg_ref.shape[1]
    keep = wide - LANE
    step = 5 * LANE
    low = lax.axis_index("dp") % 2 == 0
    for at in range(0, normed_ref.shape[1], step):
        dims = (((0,), (0,)), ((), ()))
        first = lax.dot_general(normed_ref[:, at : at + step], pg_ref[...], dims, preferred_element_type=jnp.float32)
        second = lax.dot_general(up_ref[:, at : at + step], hidden_ref[...], dims, preferred_element_type=jnp.float32)
        for b in range(0, step, 2 * block):
            m, p = divmod((at + b) // (2 * block), near)
            parts = []
            for half in (b, b + block):
                one, two = first[half : half + block] * factor, second[half : half + block] * factor
                parts.append((one[:, :keep], one[:, keep:] + two[:, :LANE], two[:, LANE:]))
            for lo, hi, start in zip(*parts, (0, keep, wide)):
                mine_ref[p, m, :, start : start + lo.shape[1]] = jnp.where(low, lo, hi).astype(jnp.bfloat16)
                theirs_ref[p, m, :, start : start + lo.shape[1]] = jnp.where(low, hi, lo).astype(jnp.bfloat16)


def grad_terms(tiles, table, normed, hidden, deriv, weight_t, factor, shape):
    slots, width = normed.shape
    rows = table.shape[1]
    _, places = tile_places(rows, width, tiles.shape[0])
    return pl.pallas_call(
        functools.partial(grads_kernel, places, factor),
        out_shape=(jax.ShapeDtypeStruct(shape, jnp.bfloat16),) * 2,
        scratch_shapes=[
            pltpu.VMEM((rows, width), jnp.bfloat16),
            pltpu.VMEM((slots, width), jnp.bfloat16),
            pltpu.VMEM((slots, hidden.shape[1]), jnp.bfloat16),
        ],
        name="grad_terms",
    )(tiles, table, normed, hidden, deriv, weight_t)


def tables_kernel(side, ranks_ref, table_ref, early_ref):
    rows = ranks_ref.shape[1]
    slots = table_ref.shape[0]
    groups = slots // SLOT_PAD
    ranks = ranks_ref[...]
    hot = lax.broadcasted_iota(jnp.int32, (groups, rows), 0) == ranks
    earlier = lax.broadcasted_iota(jnp.int32, (rows, rows), 0) < lax.broadcasted_iota(jnp.int32, (rows, rows), 1)
    before = jnp.dot(
        hot.astype(jnp.float32).astype(jnp.bfloat16),
        earlier.astype(jnp.float32).astype(jnp.bfloat16),
        preferred_element_type=jnp.float32,
    )
    position = jnp.sum(jnp.where(hot, before, 0.0), axis=0, keepdims=True).astype(jnp.int32)
    targets = lax.broadcasted_iota(jnp.int32, (slots, rows), 0)
    table_ref[...] = (targets == ranks * SLOT_PAD + position).astype(jnp.float32).astype(jnp.bfloat16)
    shift = side.bit_length() - 1
    me = lax.axis_index("tp")
    dx = ((ranks >> shift) - (me >> shift)) & (side - 1)
    dy = ((ranks & (side - 1)) - (me & (side - 1))) & (side - 1)
    x_first = lax.axis_index("dp") % 2 == 0
    where_to = jnp.where(x_first, dx * side + dy, dy * side + dx)
    early_ref[...] = (targets == where_to * SLOT_PAD + position).astype(jnp.float32).astype(jnp.bfloat16)


def slot_tables(rank_ids, groups):
    shape = jax.ShapeDtypeStruct((groups * SLOT_PAD, rank_ids.shape[1]), jnp.bfloat16)
    return pl.pallas_call(
        functools.partial(tables_kernel, int(groups**0.5)), out_shape=(shape, shape), name="slot_tables",
    )(rank_ids)


def exchange(blocks, axis, groups=None):
    return lax.all_to_all(blocks, axis, 0, 0, tiled=True, axis_index_groups=groups)


def to_all(shard, axis):
    return exchange(jnp.broadcast_to(shard, (lax.axis_size(axis), *shard.shape)), axis)


def total(arrived):
    return arrived.astype(jnp.float32).sum(axis=0).astype(jnp.bfloat16)


def plane_rounds(replicas, side):
    rounds = []
    for turn in range(2):
        perms = []
        for d in range(1, side):
            pairs = []
            for k in range(replicas):
                for x in range(side):
                    for y in range(side):
                        along_x = (k % 2 == 0) == (turn == 0)
                        to = ((x + d) % side, y) if along_x else (x, (y + d) % side)
                        pairs.append(((k * side + x) * side + y, (k * side + to[0]) * side + to[1]))
            perms.append(pairs)
        rounds.append(perms)
    return rounds


def named_permute(value, pairs):
    return lax.ppermute(value, ("dp", "tp"), pairs)


def summed(own, moved):
    return sum((b.astype(jnp.float32) for b in moved), own.astype(jnp.float32)).astype(jnp.bfloat16)


def route_early(part, table, replicas, groups):
    side = int(groups**0.5)
    rounds = plane_rounds(replicas, side)
    span = side * SLOT_PAD
    blocks = []
    for d in range(side):
        block = jnp.dot(table[d * span : (d + 1) * span], part, preferred_element_type=jnp.float32)
        blocks.append(block.astype(jnp.bfloat16))
    moved = [named_permute(blocks[d], rounds[0][d - 1]) for d in range(1, side)]
    half_way = summed(lax.optimization_barrier(blocks[0]), moved)
    pieces = [half_way[d * SLOT_PAD : (d + 1) * SLOT_PAD] for d in range(side)]
    moved = [named_permute(pieces[d], rounds[1][d - 1]) for d in range(1, side)]
    return summed(pieces[0], moved)


def dp_groups(replicas):
    cores, near = 2, 4
    depth = replicas // cores
    far = depth // near
    pairs = [(k, k ^ 1) for k in range(replicas)]
    close = []
    for g in range(far):
        close.append([cores * (near * g + p) for p in range(near)])
    for g in range(far):
        zs = [(near * (g + 1) + p) % depth if p < near // 2 else near * g + p for p in range(near)]
        close.append([cores * z + 1 for z in zs])
    strided = [[cores * (near * m + p) + c for m in range(far)] for p in range(near) for c in range(cores)]
    return cores, near, far, pairs, close, strided


def shards(partials, layer_input, ln_gain, ln_bias, fc1_weight, fc1_bias, fc2_weight, row_rank):
    groups = lax.axis_size("tp")
    replicas = lax.axis_size("dp")
    local_part = partials[0]
    row_count = local_part.shape[0]
    slot_count, width = layer_input.shape
    units = fc1_weight.shape[1]
    _, near, far, pairs, close, strided = dp_groups(replicas)
    block = width // replicas

    arrived = exchange(cut_tiles(local_part, layer_input, groups), "tp")
    head = arrived.shape[1] - (SLOT_PAD // SUB) * (width // LANE)
    own_tiles = total(arrived[:, :head])
    tiles = to_all(own_tiles, "tp")

    table, early_table = slot_tables(row_rank.T, groups)
    normed_all, hidden, derivative = hidden_parts(arrived, head, ln_gain, ln_bias, fc1_weight.T, fc1_bias)
    placed = route_early(local_part[:, width:], early_table, replicas, groups)[:slot_count]

    factor = float(replicas * row_count) ** (-0.5)
    mine, theirs = grad_terms(
        tiles, table, normed_all, hidden, derivative, fc2_weight.T, factor,
        (near, far, block, 2 * units),
    )
    theirs = lax.ppermute(theirs, "dp", pairs)
    both = summed(mine, (theirs,))
    both = exchange(both, "dp", close)
    both = total(both)
    both = exchange(both, "dp", strided)
    both = total(both)
    return (placed, both[:, :units], both[:, units:])


def solution(mesh):
    return jax.shard_map(
        shards,
        mesh=mesh,
        in_specs=(
            P("tp", "dp", None),
            P(("dp", "tp"), None),
            P(),
            P(),
            P(None, "tp"),
            P("tp"),
            P(None, "tp"),
            P("dp", None),
        ),
        out_specs=(P(("dp", "tp"), None), P("dp", "tp"), P("dp", "tp")),
        check_vma=False,
    )
```

```python
import functools

import jax
import jax.numpy as jnp
from jax import lax
from jax.experimental import pallas as pl
from jax.experimental.pallas import tpu as pltpu
from jax.sharding import PartitionSpec as P


SUB, LANE = 8, 128
SLOT_PAD = 16
GRADS_VMEM = 24


def tile_places(rows, width, parts):
    across = width // LANE
    total = (rows // SUB) * across
    whole = total // parts
    places = []
    for t in range(total):
        r, c = divmod(t, across)
        if t < whole * parts:
            places.append((*divmod(t, whole), 0, SUB, r * SUB, c * LANE))
        else:
            half = SUB // 2
            for h in range(2):
                part = 2 * (t - whole * parts) + h
                places.append((part, whole, 0, half, r * SUB + h * half, c * LANE))
    return whole + 1, places


def cut_kernel(places, x_hbm, layer_hbm, out_hbm, x_ref, layer_ref, out_ref, in_sem, out_sem):
    parts, depth = out_ref.shape[:2]
    slot_count, width = layer_ref.shape
    across = width // LANE
    head = depth - (SLOT_PAD // SUB) * across
    get_layer = pltpu.make_async_copy(layer_hbm, layer_ref, in_sem.at[0])
    get_x = pltpu.make_async_copy(x_hbm.at[:, pl.ds(0, width)], x_ref, in_sem.at[1])
    get_layer.start()
    get_x.start()
    get_layer.wait()
    for at in range(0, SLOT_PAD, SUB):
        size = min(SUB, slot_count - at)
        for c in range(across):
            tile = layer_ref[at : at + size, c * LANE : (c + 1) * LANE]
            for part in range(parts):
                out_ref[part, head + (at // SUB) * across + c, :size, :] = tile
                if size < SUB:
                    out_ref[part, head + (at // SUB) * across + c, size:, :] = jnp.zeros((SUB - size, LANE), tile.dtype)
    rest = pl.ds(head, depth - head)
    put_layer = pltpu.make_async_copy(out_ref.at[:, rest], out_hbm.at[:, rest], out_sem.at[0])
    put_layer.start()
    get_x.wait()
    for part, i, at, size, r, c in places:
        out_ref[part, i, at : at + size, :] = x_ref[r : r + size, c : c + LANE]
        if size < SUB:
            out_ref[part, i, size:, :] = jnp.zeros((SUB - size, LANE), out_ref.dtype)
    some = pl.ds(0, head)
    put_x = pltpu.make_async_copy(out_ref.at[:, some], out_hbm.at[:, some], out_sem.at[1])
    put_x.start()
    put_layer.wait()
    put_x.wait()


def cut_tiles(x, layer, parts):
    rows, width = x.shape[0], layer.shape[1]
    depth, places = tile_places(rows, width, parts)
    depth += (SLOT_PAD // SUB) * (width // LANE)
    anywhere = pl.BlockSpec(memory_space=pl.ANY)
    return pl.pallas_call(
        functools.partial(cut_kernel, places),
        in_specs=[anywhere] * 2,
        out_specs=anywhere,
        out_shape=jax.ShapeDtypeStruct((parts, depth, SUB, LANE), x.dtype),
        scratch_shapes=[
            pltpu.VMEM((rows, width), x.dtype),
            pltpu.VMEM(layer.shape, x.dtype),
            pltpu.VMEM((parts, depth, SUB, LANE), x.dtype),
            pltpu.SemaphoreType.DMA((2,)),
            pltpu.SemaphoreType.DMA((2,)),
        ],
        name="cut_tiles",
    )(x, layer)


def gelu_parts(preact):
    normal_cdf = 0.5 * (1.0 + lax.erf(preact * 0.7071067811865476))
    density = jnp.exp(-0.5 * preact * preact) * 0.3989422804014327
    return (preact * normal_cdf, normal_cdf + preact * density)


def hidden_kernel(head, tiles_ref, gain_ref, bias_ref, weight_ref, fc1_bias_ref, packed_ref):
    parts = tiles_ref.shape[0]
    slots = packed_ref.shape[0]
    units, width = weight_ref.shape
    wide = -(-units // LANE) * LANE
    across = width // LANE
    per_part = slots // parts
    for part in range(parts):
        for at in range(0, per_part, SUB):
            for c in range(across):
                packed_ref[part * per_part + at : part * per_part + at + SUB, c * LANE : (c + 1) * LANE] = tiles_ref[
                    part, head + (at // SUB) * across + c
                ]
    values = packed_ref[:, :width].astype(jnp.float32)
    centered = values - jnp.mean(values, axis=1, keepdims=True)
    row_var = jnp.mean(centered * centered, axis=1, keepdims=True)
    normed = (centered / jnp.sqrt(row_var + 1e-05) * gain_ref[...][None] + bias_ref[...][None]).astype(jnp.bfloat16)
    packed_ref[:, :width] = normed
    preact = lax.dot_general(normed, weight_ref[...], (((1,), (1,)), ((), ())), preferred_element_type=jnp.float32)
    activated, derivative = gelu_parts(preact + fc1_bias_ref[...][None])
    packed_ref[:, width:] = jnp.zeros((slots, 2 * wide), jnp.bfloat16)
    packed_ref[:, width + wide - units : width + wide] = activated.astype(jnp.bfloat16)
    packed_ref[:, width + wide : width + wide + units] = derivative.astype(jnp.bfloat16)


def hidden_parts(tiles, head, gain, bias, weight_t, fc1_bias):
    units, width = weight_t.shape
    slots = tiles.shape[0] * SLOT_PAD
    wide = -(-units // LANE) * LANE
    return pl.pallas_call(
        functools.partial(hidden_kernel, head),
        out_shape=jax.ShapeDtypeStruct((slots, width + 2 * wide), jnp.bfloat16),
        name="hidden_parts",
    )(tiles, gain, bias, weight_t, fc1_bias)


def grads_kernel(places, factor, *refs):
    sources, (mine_hbm, theirs_hbm), scratch = refs[:4], refs[4:6], refs[6:]
    tiles_ref, table_ref, weight_ref, packed_ref = scratch[:4]
    mine_ref, theirs_ref, rows_ref, up_ref, pg_ref, in_sem, out_sem = scratch[4:]
    width = up_ref.shape[1]
    loads = [pltpu.make_async_copy(src, dst, in_sem.at[i]) for i, (src, dst) in enumerate(zip(sources, scratch[:4]))]
    for load in loads:
        load.start()
    loads[0].wait()
    for part, i, at, size, r, c in places:
        rows_ref[r : r + size, c : c + LANE] = tiles_ref[part, i, at : at + size, :]
    loads[1].wait()
    up_ref[...] = jnp.dot(table_ref[...], rows_ref[...], preferred_element_type=jnp.float32).astype(jnp.bfloat16)
    loads[2].wait()
    hidden_grad = lax.dot_general(
        up_ref[...], weight_ref[...], (((1,), (1,)), ((), ())), preferred_element_type=jnp.float32
    )
    units = hidden_grad.shape[1]
    loads[3].wait()
    deriv_at = width + pg_ref.shape[1]
    pg_ref[...] = jnp.zeros_like(pg_ref)
    pg_ref[:, :units] = (hidden_grad * packed_ref[:, deriv_at : deriv_at + units].astype(jnp.float32)).astype(jnp.bfloat16)
    near, far, block, _ = mine_ref.shape
    wide = pg_ref.shape[1]
    keep = wide - LANE
    halves = 2
    step = width // halves
    low = lax.axis_index("dp") % 2 == 0
    stores = []
    for turn in range(halves):
        at = turn * step
        dims = (((0,), (0,)), ((), ()))
        first = lax.dot_general(packed_ref[:, at : at + step], pg_ref[...], dims, preferred_element_type=jnp.float32)
        hidden = packed_ref[:, width : width + wide]
        second = lax.dot_general(up_ref[:, at : at + step], hidden, dims, preferred_element_type=jnp.float32)
        for b in range(0, step, 2 * block):
            m, p = divmod((at + b) // (2 * block), near)
            parts = []
            for half in (b, b + block):
                one, two = first[half : half + block] * factor, second[half : half + block] * factor
                parts.append((one[:, :keep], one[:, keep:] + two[:, :LANE], two[:, LANE:]))
            for lo, hi, start in zip(*parts, (0, keep, wide)):
                mine_ref[p, m, :, start : start + lo.shape[1]] = jnp.where(low, lo, hi).astype(jnp.bfloat16)
                theirs_ref[p, m, :, start : start + lo.shape[1]] = jnp.where(low, hi, lo).astype(jnp.bfloat16)
        some = pl.ds(turn * (far // halves), far // halves)
        for j, (src, dst) in enumerate(((theirs_ref, theirs_hbm), (mine_ref, mine_hbm))):
            store = pltpu.make_async_copy(src.at[:, some], dst.at[:, some], out_sem.at[2 * turn + j])
            store.start()
            stores.append(store)
    for store in stores:
        store.wait()


def grad_terms(tiles, table, packed, weight_t, factor, shape):
    units, width = weight_t.shape
    slots, rows = table.shape
    wide = -(-units // LANE) * LANE
    _, places = tile_places(rows, width, tiles.shape[0])
    operands = (tiles, table, weight_t, packed)
    anywhere = pl.BlockSpec(memory_space=pl.ANY)
    return pl.pallas_call(
        functools.partial(grads_kernel, places, factor),
        in_specs=[anywhere] * len(operands),
        out_specs=(anywhere,) * 2,
        out_shape=(jax.ShapeDtypeStruct(shape, jnp.bfloat16),) * 2,
        scratch_shapes=[pltpu.VMEM(a.shape, a.dtype) for a in operands]
        + [
            pltpu.VMEM(shape, jnp.bfloat16),
            pltpu.VMEM(shape, jnp.bfloat16),
            pltpu.VMEM((rows, width), jnp.bfloat16),
            pltpu.VMEM((slots, width), jnp.bfloat16),
            pltpu.VMEM((slots, wide), jnp.bfloat16),
            pltpu.SemaphoreType.DMA((len(operands),)),
            pltpu.SemaphoreType.DMA((4,)),
        ],
        name="grad_terms",
        compiler_params=pltpu.CompilerParams(vmem_limit_bytes=GRADS_VMEM << 20),
    )(*operands)


def tables_kernel(side, ranks_ref, table_ref, early_ref):
    rows = ranks_ref.shape[1]
    slots = table_ref.shape[0]
    groups = slots // SLOT_PAD
    ranks = ranks_ref[...]
    hot = lax.broadcasted_iota(jnp.int32, (groups, rows), 0) == ranks
    earlier = lax.broadcasted_iota(jnp.int32, (rows, rows), 0) < lax.broadcasted_iota(jnp.int32, (rows, rows), 1)
    before = jnp.dot(
        hot.astype(jnp.float32).astype(jnp.bfloat16),
        earlier.astype(jnp.float32).astype(jnp.bfloat16),
        preferred_element_type=jnp.float32,
    )
    position = jnp.sum(jnp.where(hot, before, 0.0), axis=0, keepdims=True).astype(jnp.int32)
    targets = lax.broadcasted_iota(jnp.int32, (slots, rows), 0)
    table_ref[...] = (targets == ranks * SLOT_PAD + position).astype(jnp.float32).astype(jnp.bfloat16)
    shift = side.bit_length() - 1
    me = lax.axis_index("tp")
    dx = ((ranks >> shift) - (me >> shift)) & (side - 1)
    dy = ((ranks & (side - 1)) - (me & (side - 1))) & (side - 1)
    x_first = lax.axis_index("dp") % 2 == 0
    where_to = jnp.where(x_first, dx * side + dy, dy * side + dx)
    early_ref[...] = (targets == where_to * SLOT_PAD + position).astype(jnp.float32).astype(jnp.bfloat16)


def slot_tables(rank_ids, groups):
    shape = jax.ShapeDtypeStruct((groups * SLOT_PAD, rank_ids.shape[1]), jnp.bfloat16)
    return pl.pallas_call(
        functools.partial(tables_kernel, int(groups**0.5)), out_shape=(shape, shape), name="slot_tables",
    )(rank_ids)


def exchange(blocks, axis, groups=None):
    return lax.all_to_all(blocks, axis, 0, 0, tiled=True, axis_index_groups=groups)


def to_all(shard, axis):
    return exchange(jnp.broadcast_to(shard, (lax.axis_size(axis), *shard.shape)), axis)


def total(arrived):
    return arrived.astype(jnp.float32).sum(axis=0).astype(jnp.bfloat16)


def plane_rounds(replicas, side):
    rounds = []
    for turn in range(2):
        perms = []
        for d in range(1, side):
            pairs = []
            for k in range(replicas):
                for x in range(side):
                    for y in range(side):
                        along_x = (k % 2 == 0) == (turn == 0)
                        to = ((x + d) % side, y) if along_x else (x, (y + d) % side)
                        pairs.append(((k * side + x) * side + y, (k * side + to[0]) * side + to[1]))
            perms.append(pairs)
        rounds.append(perms)
    return rounds


def named_permute(value, pairs):
    return lax.ppermute(value, ("dp", "tp"), pairs)


def summed(own, moved):
    return sum((b.astype(jnp.float32) for b in moved), own.astype(jnp.float32)).astype(jnp.bfloat16)


def route_early(part, table, replicas, groups):
    side = int(groups**0.5)
    rounds = plane_rounds(replicas, side)
    span = side * SLOT_PAD
    blocks = []
    for d in range(side):
        block = jnp.dot(table[d * span : (d + 1) * span], part, preferred_element_type=jnp.float32)
        blocks.append(block.astype(jnp.bfloat16))
    moved = [named_permute(blocks[d], rounds[0][d - 1]) for d in range(1, side)]
    half_way = summed(lax.optimization_barrier(blocks[0]), moved)
    pieces = [half_way[d * SLOT_PAD : (d + 1) * SLOT_PAD] for d in range(side)]
    moved = [named_permute(pieces[d], rounds[1][d - 1]) for d in range(1, side)]
    return summed(pieces[0], moved)


def dp_groups(replicas):
    cores, near = 2, 4
    depth = replicas // cores
    far = depth // near
    pairs = [(k, k ^ 1) for k in range(replicas)]
    close = []
    for g in range(far):
        close.append([cores * (near * g + p) for p in range(near)])
    for g in range(far):
        zs = [(near * (g + 1) + p) % depth if p < near // 2 else near * g + p for p in range(near)]
        close.append([cores * z + 1 for z in zs])
    strided = [[cores * (near * m + p) + c for m in range(far)] for p in range(near) for c in range(cores)]
    return cores, near, far, pairs, close, strided


def shards(partials, layer_input, ln_gain, ln_bias, fc1_weight, fc1_bias, fc2_weight, row_rank):
    groups = lax.axis_size("tp")
    replicas = lax.axis_size("dp")
    local_part = partials[0]
    row_count = local_part.shape[0]
    slot_count, width = layer_input.shape
    units = fc1_weight.shape[1]
    _, near, far, pairs, close, strided = dp_groups(replicas)
    block = width // replicas

    arrived = exchange(cut_tiles(local_part, layer_input, groups), "tp")
    head = arrived.shape[1] - (SLOT_PAD // SUB) * (width // LANE)
    own_tiles = total(arrived[:, :head])
    tiles = to_all(own_tiles, "tp")

    table, early_table = slot_tables(row_rank.T, groups)
    packed = hidden_parts(arrived, head, ln_gain, ln_bias, fc1_weight.T, fc1_bias)
    placed = route_early(local_part[:, width:], early_table, replicas, groups)[:slot_count]

    factor = float(replicas * row_count) ** (-0.5)
    mine, theirs = grad_terms(
        tiles, table, packed, fc2_weight.T, factor,
        (near, far, block, 2 * units),
    )
    theirs = lax.ppermute(theirs, "dp", pairs)
    both = summed(mine, (theirs,))
    both = exchange(both, "dp", close)
    both = total(both)
    both = exchange(both, "dp", strided)
    both = total(both)
    first, second = both[:, :units], both[:, units:]
    return (placed, first, second)


def solution(mesh):
    return jax.shard_map(
        shards,
        mesh=mesh,
        in_specs=(
            P("tp", "dp", None),
            P(("dp", "tp"), None),
            P(),
            P(),
            P(None, "tp"),
            P("tp"),
            P(None, "tp"),
            P("dp", None),
        ),
        out_specs=(P(("dp", "tp"), None), P("dp", "tp"), P("dp", "tp")),
        check_vma=False,
    )
```

```python
import functools

import jax
import jax.numpy as jnp
from jax import lax
from jax.experimental import pallas as pl
from jax.experimental.pallas import tpu as pltpu
from jax.sharding import PartitionSpec as P


SUB, LANE = 8, 128
SLOT_PAD = 16
GRADS_VMEM = 24


def tile_places(rows, width, parts):
    across = width // LANE
    total = (rows // SUB) * across
    whole = total // parts
    places = []
    for t in range(total):
        r, c = divmod(t, across)
        if t < whole * parts:
            places.append((*divmod(t, whole), 0, SUB, r * SUB, c * LANE))
        else:
            half = SUB // 2
            for h in range(2):
                part = 2 * (t - whole * parts) + h
                places.append((part, whole, 0, half, r * SUB + h * half, c * LANE))
    return whole + 1, places


def cut_kernel(places, x_hbm, layer_hbm, out_hbm, x_ref, layer_ref, out_ref, in_sem, out_sem):
    parts, depth = out_ref.shape[:2]
    slot_count, width = layer_ref.shape
    across = width // LANE
    head = depth - (SLOT_PAD // SUB) * across
    get_layer = pltpu.make_async_copy(layer_hbm, layer_ref, in_sem.at[0])
    get_x = pltpu.make_async_copy(x_hbm.at[:, pl.ds(0, width)], x_ref, in_sem.at[1])
    get_layer.start()
    get_x.start()
    get_layer.wait()
    for at in range(0, SLOT_PAD, SUB):
        size = min(SUB, slot_count - at)
        for c in range(across):
            tile = layer_ref[at : at + size, c * LANE : (c + 1) * LANE]
            for part in range(parts):
                out_ref[part, head + (at // SUB) * across + c, :size, :] = tile
                if size < SUB:
                    out_ref[part, head + (at // SUB) * across + c, size:, :] = jnp.zeros((SUB - size, LANE), tile.dtype)
    rest = pl.ds(head, depth - head)
    put_layer = pltpu.make_async_copy(out_ref.at[:, rest], out_hbm.at[:, rest], out_sem.at[0])
    put_layer.start()
    get_x.wait()
    for part, i, at, size, r, c in places:
        out_ref[part, i, at : at + size, :] = x_ref[r : r + size, c : c + LANE]
        if size < SUB:
            out_ref[part, i, size:, :] = jnp.zeros((SUB - size, LANE), out_ref.dtype)
    some = pl.ds(0, head)
    put_x = pltpu.make_async_copy(out_ref.at[:, some], out_hbm.at[:, some], out_sem.at[1])
    put_x.start()
    put_layer.wait()
    put_x.wait()


def cut_tiles(x, layer, parts):
    rows, width = x.shape[0], layer.shape[1]
    depth, places = tile_places(rows, width, parts)
    depth += (SLOT_PAD // SUB) * (width // LANE)
    anywhere = pl.BlockSpec(memory_space=pl.ANY)
    return pl.pallas_call(
        functools.partial(cut_kernel, places),
        in_specs=[anywhere] * 2,
        out_specs=anywhere,
        out_shape=jax.ShapeDtypeStruct((parts, depth, SUB, LANE), x.dtype),
        scratch_shapes=[
            pltpu.VMEM((rows, width), x.dtype),
            pltpu.VMEM(layer.shape, x.dtype),
            pltpu.VMEM((parts, depth, SUB, LANE), x.dtype),
            pltpu.SemaphoreType.DMA((2,)),
            pltpu.SemaphoreType.DMA((2,)),
        ],
        name="cut_tiles",
    )(x, layer)


def gelu_parts(preact):
    normal_cdf = 0.5 * (1.0 + lax.erf(preact * 0.7071067811865476))
    density = jnp.exp(-0.5 * preact * preact) * 0.3989422804014327
    return (preact * normal_cdf, normal_cdf + preact * density)


def hidden_kernel(head, tiles_ref, gain_ref, bias_ref, weight_ref, fc1_bias_ref, table_ref, packed_ref):
    parts = tiles_ref.shape[0]
    slots = packed_ref.shape[0]
    units, width = weight_ref.shape
    wide = -(-units // LANE) * LANE
    across = width // LANE
    per_part = slots // parts
    for part in range(parts):
        for at in range(0, per_part, SUB):
            for c in range(across):
                packed_ref[part * per_part + at : part * per_part + at + SUB, c * LANE : (c + 1) * LANE] = tiles_ref[
                    part, head + (at // SUB) * across + c
                ]
    values = packed_ref[:, :width].astype(jnp.float32)
    centered = values - jnp.mean(values, axis=1, keepdims=True)
    row_var = jnp.mean(centered * centered, axis=1, keepdims=True)
    normed = (centered / jnp.sqrt(row_var + 1e-05) * gain_ref[...][None] + bias_ref[...][None]).astype(jnp.bfloat16)
    packed_ref[:, :width] = normed
    preact = lax.dot_general(normed, weight_ref[...], (((1,), (1,)), ((), ())), preferred_element_type=jnp.float32)
    activated, derivative = gelu_parts(preact + fc1_bias_ref[...][None])
    packed_ref[:, width:] = jnp.zeros((slots, packed_ref.shape[1] - width), jnp.bfloat16)
    packed_ref[:, width + 2 * wide : width + 2 * wide + table_ref.shape[1]] = table_ref[...]
    packed_ref[:, width + wide - units : width + wide] = activated.astype(jnp.bfloat16)
    packed_ref[:, width + wide : width + wide + units] = derivative.astype(jnp.bfloat16)


def hidden_parts(tiles, head, gain, bias, weight_t, fc1_bias, table):
    units, width = weight_t.shape
    slots = tiles.shape[0] * SLOT_PAD
    wide = -(-units // LANE) * LANE
    spare = -(-table.shape[1] // LANE) * LANE
    return pl.pallas_call(
        functools.partial(hidden_kernel, head),
        out_shape=jax.ShapeDtypeStruct((slots, width + 2 * wide + spare), jnp.bfloat16),
        name="hidden_parts",
        compiler_params=pltpu.CompilerParams(vmem_limit_bytes=16 << 20),
    )(tiles, gain, bias, weight_t, fc1_bias, table)


def grads_kernel(places, factor, *refs):
    sources, (mine_hbm, theirs_hbm), scratch = refs[:3], refs[3:5], refs[5:]
    tiles_ref, packed_ref, weight_ref = scratch[:3]
    mine_ref, theirs_ref, rows_ref, up_ref, pg_ref, in_sem, out_sem = scratch[3:]
    width = up_ref.shape[1]
    loads = [pltpu.make_async_copy(src, dst, in_sem.at[i]) for i, (src, dst) in enumerate(zip(sources, scratch[:3]))]
    for load in loads:
        load.start()
    loads[0].wait()
    for part, i, at, size, r, c in places:
        rows_ref[r : r + size, c : c + LANE] = tiles_ref[part, i, at : at + size, :]
    loads[1].wait()
    table_at = width + 2 * pg_ref.shape[1]
    table = packed_ref[:, table_at : table_at + rows_ref.shape[0]]
    up_ref[...] = jnp.dot(table, rows_ref[...], preferred_element_type=jnp.float32).astype(jnp.bfloat16)
    loads[2].wait()
    hidden_grad = lax.dot_general(
        up_ref[...], weight_ref[...], (((1,), (1,)), ((), ())), preferred_element_type=jnp.float32
    )
    units = hidden_grad.shape[1]
    deriv_at = width + pg_ref.shape[1]
    pg_ref[...] = jnp.zeros_like(pg_ref)
    pg_ref[:, :units] = (hidden_grad * packed_ref[:, deriv_at : deriv_at + units].astype(jnp.float32)).astype(jnp.bfloat16)
    near, far, block, _ = mine_ref.shape
    wide = pg_ref.shape[1]
    keep = wide - LANE
    halves = 2
    step = width // halves
    low = lax.axis_index("dp") % 2 == 0
    stores = []
    for turn in range(halves):
        at = turn * step
        dims = (((0,), (0,)), ((), ()))
        first = lax.dot_general(packed_ref[:, at : at + step], pg_ref[...], dims, preferred_element_type=jnp.float32)
        hidden = packed_ref[:, width : width + wide]
        second = lax.dot_general(up_ref[:, at : at + step], hidden, dims, preferred_element_type=jnp.float32)
        for b in range(0, step, 2 * block):
            m, p = divmod((at + b) // (2 * block), near)
            parts = []
            for half in (b, b + block):
                one, two = first[half : half + block] * factor, second[half : half + block] * factor
                parts.append((one[:, :keep], one[:, keep:] + two[:, :LANE], two[:, LANE:]))
            for lo, hi, start in zip(*parts, (0, keep, wide)):
                mine_ref[p, m, :, start : start + lo.shape[1]] = jnp.where(low, lo, hi).astype(jnp.bfloat16)
                theirs_ref[p, m, :, start : start + lo.shape[1]] = jnp.where(low, hi, lo).astype(jnp.bfloat16)
        some = pl.ds(turn * (far // halves), far // halves)
        for j, (src, dst) in enumerate(((theirs_ref, theirs_hbm), (mine_ref, mine_hbm))):
            store = pltpu.make_async_copy(src.at[:, some], dst.at[:, some], out_sem.at[2 * turn + j])
            store.start()
            stores.append(store)
    for store in stores:
        store.wait()


def grad_terms(tiles, packed, weight_t, rows, factor, shape):
    units, width = weight_t.shape
    slots = packed.shape[0]
    wide = -(-units // LANE) * LANE
    _, places = tile_places(rows, width, tiles.shape[0])
    operands = (tiles, packed, weight_t)
    anywhere = pl.BlockSpec(memory_space=pl.ANY)
    return pl.pallas_call(
        functools.partial(grads_kernel, places, factor),
        in_specs=[anywhere] * len(operands),
        out_specs=(anywhere,) * 2,
        out_shape=(jax.ShapeDtypeStruct(shape, jnp.bfloat16),) * 2,
        scratch_shapes=[pltpu.VMEM(a.shape, a.dtype) for a in operands]
        + [
            pltpu.VMEM(shape, jnp.bfloat16),
            pltpu.VMEM(shape, jnp.bfloat16),
            pltpu.VMEM((rows, width), jnp.bfloat16),
            pltpu.VMEM((slots, width), jnp.bfloat16),
            pltpu.VMEM((slots, wide), jnp.bfloat16),
            pltpu.SemaphoreType.DMA((len(operands),)),
            pltpu.SemaphoreType.DMA((4,)),
        ],
        name="grad_terms",
        compiler_params=pltpu.CompilerParams(vmem_limit_bytes=GRADS_VMEM << 20),
    )(*operands)


def tables_kernel(side, ranks_ref, table_ref, early_ref):
    rows = ranks_ref.shape[1]
    slots = table_ref.shape[0]
    groups = slots // SLOT_PAD
    ranks = ranks_ref[...]
    hot = lax.broadcasted_iota(jnp.int32, (groups, rows), 0) == ranks
    earlier = lax.broadcasted_iota(jnp.int32, (rows, rows), 0) < lax.broadcasted_iota(jnp.int32, (rows, rows), 1)
    before = jnp.dot(
        hot.astype(jnp.float32).astype(jnp.bfloat16),
        earlier.astype(jnp.float32).astype(jnp.bfloat16),
        preferred_element_type=jnp.float32,
    )
    position = jnp.sum(jnp.where(hot, before, 0.0), axis=0, keepdims=True).astype(jnp.int32)
    targets = lax.broadcasted_iota(jnp.int32, (slots, rows), 0)
    table_ref[...] = (targets == ranks * SLOT_PAD + position).astype(jnp.float32).astype(jnp.bfloat16)
    shift = side.bit_length() - 1
    me = lax.axis_index("tp")
    dx = ((ranks >> shift) - (me >> shift)) & (side - 1)
    dy = ((ranks & (side - 1)) - (me & (side - 1))) & (side - 1)
    x_first = lax.axis_index("dp") % 2 == 0
    where_to = jnp.where(x_first, dx * side + dy, dy * side + dx)
    early_ref[...] = (targets == where_to * SLOT_PAD + position).astype(jnp.float32).astype(jnp.bfloat16)


def slot_tables(rank_ids, groups):
    shape = jax.ShapeDtypeStruct((groups * SLOT_PAD, rank_ids.shape[1]), jnp.bfloat16)
    return pl.pallas_call(
        functools.partial(tables_kernel, int(groups**0.5)), out_shape=(shape, shape), name="slot_tables",
    )(rank_ids)


def exchange(blocks, axis, groups=None):
    return lax.all_to_all(blocks, axis, 0, 0, tiled=True, axis_index_groups=groups)


def to_all(shard, axis):
    return exchange(jnp.broadcast_to(shard, (lax.axis_size(axis), *shard.shape)), axis)


def total(arrived):
    return arrived.astype(jnp.float32).sum(axis=0).astype(jnp.bfloat16)


def plane_rounds(replicas, side):
    rounds = []
    for turn in range(2):
        perms = []
        for d in range(1, side):
            pairs = []
            for k in range(replicas):
                for x in range(side):
                    for y in range(side):
                        along_x = (k % 2 == 0) == (turn == 0)
                        to = ((x + d) % side, y) if along_x else (x, (y + d) % side)
                        pairs.append(((k * side + x) * side + y, (k * side + to[0]) * side + to[1]))
            perms.append(pairs)
        rounds.append(perms)
    return rounds


def named_permute(value, pairs):
    return lax.ppermute(value, ("dp", "tp"), pairs)


def summed(own, moved):
    return sum((b.astype(jnp.float32) for b in moved), own.astype(jnp.float32)).astype(jnp.bfloat16)


def route_early(part, table, replicas, groups):
    side = int(groups**0.5)
    rounds = plane_rounds(replicas, side)
    span = side * SLOT_PAD
    blocks = []
    for d in range(side):
        block = jnp.dot(table[d * span : (d + 1) * span], part, preferred_element_type=jnp.float32)
        blocks.append(block.astype(jnp.bfloat16))
    moved = [named_permute(blocks[d], rounds[0][d - 1]) for d in range(1, side)]
    half_way = summed(lax.optimization_barrier(blocks[0]), moved)
    pieces = [half_way[d * SLOT_PAD : (d + 1) * SLOT_PAD] for d in range(side)]
    moved = [named_permute(pieces[d], rounds[1][d - 1]) for d in range(1, side)]
    return summed(pieces[0], moved)


def dp_groups(replicas):
    cores, near = 2, 4
    depth = replicas // cores
    far = depth // near
    pairs = [(k, k ^ 1) for k in range(replicas)]
    close = []
    for g in range(far):
        close.append([cores * (near * g + p) for p in range(near)])
    for g in range(far):
        zs = [(near * (g + 1) + p) % depth if p < near // 2 else near * g + p for p in range(near)]
        close.append([cores * z + 1 for z in zs])
    strided = [[cores * (near * m + p) + c for m in range(far)] for p in range(near) for c in range(cores)]
    return cores, near, far, pairs, close, strided


def shards(partials, layer_input, ln_gain, ln_bias, fc1_weight, fc1_bias, fc2_weight, row_rank):
    groups = lax.axis_size("tp")
    replicas = lax.axis_size("dp")
    local_part = partials[0]
    row_count = local_part.shape[0]
    slot_count, width = layer_input.shape
    units = fc1_weight.shape[1]
    _, near, far, pairs, close, strided = dp_groups(replicas)
    block = width // replicas

    arrived = exchange(cut_tiles(local_part, layer_input, groups), "tp")
    head = arrived.shape[1] - (SLOT_PAD // SUB) * (width // LANE)
    own_tiles = total(arrived[:, :head])
    tiles = to_all(own_tiles, "tp")

    table, early_table = slot_tables(row_rank.T, groups)
    packed = hidden_parts(arrived, head, ln_gain, ln_bias, fc1_weight.T, fc1_bias, table)
    placed = route_early(local_part[:, width:], early_table, replicas, groups)[:slot_count]

    factor = float(replicas * row_count) ** (-0.5)
    mine, theirs = grad_terms(
        tiles, packed, fc2_weight.T, row_count, factor,
        (near, far, block, 2 * units),
    )
    theirs = lax.ppermute(theirs, "dp", pairs)
    both = summed(mine, (theirs,))
    both = exchange(both, "dp", close)
    both = total(both)
    both = exchange(both, "dp", strided)
    both = total(both)
    first, second = both[:, :units], both[:, units:]
    return (placed, first, second)


def solution(mesh):
    return jax.shard_map(
        shards,
        mesh=mesh,
        in_specs=(
            P("tp", "dp", None),
            P(("dp", "tp"), None),
            P(),
            P(),
            P(None, "tp"),
            P("tp"),
            P(None, "tp"),
            P("dp", None),
        ),
        out_specs=(P(("dp", "tp"), None), P("dp", "tp"), P("dp", "tp")),
        check_vma=False,
    )
```

```python
import functools

import jax
import jax.numpy as jnp
from jax import lax
from jax.experimental import pallas as pl
from jax.experimental.pallas import tpu as pltpu
from jax.sharding import PartitionSpec as P


SUB, LANE = 8, 128
SLOT_PAD = 16
GRADS_VMEM = 24


def tile_places(rows, width, parts):
    across = width // LANE
    total = (rows // SUB) * across
    whole = total // parts
    places = []
    for t in range(total):
        r, c = divmod(t, across)
        if t < whole * parts:
            places.append((*divmod(t, whole), 0, SUB, r * SUB, c * LANE))
        else:
            half = SUB // 2
            for h in range(2):
                part = 2 * (t - whole * parts) + h
                places.append((part, whole, 0, half, r * SUB + h * half, c * LANE))
    return whole + 1, places


def cut_kernel(places, x_hbm, layer_hbm, out_hbm, x_ref, layer_ref, out_ref, in_sem, out_sem):
    parts, depth = out_ref.shape[:2]
    slot_count, width = layer_ref.shape
    across = width // LANE
    head = depth - (SLOT_PAD // SUB) * across
    get_layer = pltpu.make_async_copy(layer_hbm, layer_ref, in_sem.at[0])
    get_x = pltpu.make_async_copy(x_hbm.at[:, pl.ds(0, width)], x_ref, in_sem.at[1])
    get_layer.start()
    get_x.start()
    get_layer.wait()
    for at in range(0, SLOT_PAD, SUB):
        size = min(SUB, slot_count - at)
        for c in range(across):
            tile = layer_ref[at : at + size, c * LANE : (c + 1) * LANE]
            for part in range(parts):
                out_ref[part, head + (at // SUB) * across + c, :size, :] = tile
                if size < SUB:
                    out_ref[part, head + (at // SUB) * across + c, size:, :] = jnp.zeros((SUB - size, LANE), tile.dtype)
    rest = pl.ds(head, depth - head)
    put_layer = pltpu.make_async_copy(out_ref.at[:, rest], out_hbm.at[:, rest], out_sem.at[0])
    put_layer.start()
    get_x.wait()
    for part, i, at, size, r, c in places:
        out_ref[part, i, at : at + size, :] = x_ref[r : r + size, c : c + LANE]
        if size < SUB:
            out_ref[part, i, size:, :] = jnp.zeros((SUB - size, LANE), out_ref.dtype)
    some = pl.ds(0, head)
    put_x = pltpu.make_async_copy(out_ref.at[:, some], out_hbm.at[:, some], out_sem.at[1])
    put_x.start()
    put_layer.wait()
    put_x.wait()


def cut_tiles(x, layer, parts):
    rows, width = x.shape[0], layer.shape[1]
    depth, places = tile_places(rows, width, parts)
    depth += (SLOT_PAD // SUB) * (width // LANE)
    anywhere = pl.BlockSpec(memory_space=pl.ANY)
    return pl.pallas_call(
        functools.partial(cut_kernel, places),
        in_specs=[anywhere] * 2,
        out_specs=anywhere,
        out_shape=jax.ShapeDtypeStruct((parts, depth, SUB, LANE), x.dtype),
        scratch_shapes=[
            pltpu.VMEM((rows, width), x.dtype),
            pltpu.VMEM(layer.shape, x.dtype),
            pltpu.VMEM((parts, depth, SUB, LANE), x.dtype),
            pltpu.SemaphoreType.DMA((2,)),
            pltpu.SemaphoreType.DMA((2,)),
        ],
        name="cut_tiles",
    )(x, layer)


def gelu_parts(preact):
    normal_cdf = 0.5 * (1.0 + lax.erf(preact * 0.7071067811865476))
    density = jnp.exp(-0.5 * preact * preact) * 0.3989422804014327
    return (preact * normal_cdf, normal_cdf + preact * density)


def hidden_kernel(head, tiles_ref, gain_ref, bias_ref, weight_ref, fc1_bias_ref, table_ref, later_ref, packed_ref):
    parts = tiles_ref.shape[0]
    slots = table_ref.shape[0]
    units, width = weight_ref.shape
    wide = -(-units // LANE) * LANE
    across = width // LANE
    per_part = slots // parts
    later_at = packed_ref.shape[1] - width
    packed_ref[:units, later_at:] = later_ref[...]
    for part in range(parts):
        for at in range(0, per_part, SUB):
            for c in range(across):
                packed_ref[part * per_part + at : part * per_part + at + SUB, c * LANE : (c + 1) * LANE] = tiles_ref[
                    part, head + (at // SUB) * across + c
                ]
    values = packed_ref[:slots, :width].astype(jnp.float32)
    centered = values - jnp.mean(values, axis=1, keepdims=True)
    row_var = jnp.mean(centered * centered, axis=1, keepdims=True)
    normed = (centered / jnp.sqrt(row_var + 1e-05) * gain_ref[...][None] + bias_ref[...][None]).astype(jnp.bfloat16)
    packed_ref[:slots, :width] = normed
    preact = lax.dot_general(normed, weight_ref[...], (((1,), (1,)), ((), ())), preferred_element_type=jnp.float32)
    activated, derivative = gelu_parts(preact + fc1_bias_ref[...][None])
    packed_ref[:slots, width:later_at] = jnp.zeros((slots, later_at - width), jnp.bfloat16)
    packed_ref[:slots, width + 2 * wide : width + 2 * wide + table_ref.shape[1]] = table_ref[...]
    packed_ref[:slots, width + wide - units : width + wide] = activated.astype(jnp.bfloat16)
    packed_ref[:slots, width + wide : width + wide + units] = derivative.astype(jnp.bfloat16)


def hidden_parts(tiles, head, gain, bias, weight_t, fc1_bias, table, later):
    units, width = weight_t.shape
    slots = tiles.shape[0] * SLOT_PAD
    wide = -(-units // LANE) * LANE
    spare = -(-table.shape[1] // LANE) * LANE
    return pl.pallas_call(
        functools.partial(hidden_kernel, head),
        out_shape=jax.ShapeDtypeStruct((max(slots, units), 2 * width + 2 * wide + spare), jnp.bfloat16),
        name="hidden_parts",
        compiler_params=pltpu.CompilerParams(vmem_limit_bytes=16 << 20),
    )(tiles, gain, bias, weight_t, fc1_bias, table, later)


def grads_kernel(places, factor, units, tiles_ref, packed_ref, mine_ref, theirs_ref, rows_ref, up_ref, pg_ref):
    rows, width = rows_ref.shape
    slots, wide = pg_ref.shape
    later_at = packed_ref.shape[1] - width
    for part, i, at, size, r, c in places:
        rows_ref[r : r + size, c : c + LANE] = tiles_ref[part, i, at : at + size, :]
    table = packed_ref[:slots, width + 2 * wide : width + 2 * wide + rows]
    up_ref[...] = jnp.dot(table, rows_ref[...], preferred_element_type=jnp.float32).astype(jnp.bfloat16)
    hidden_grad = lax.dot_general(
        up_ref[...], packed_ref[:units, later_at:], (((1,), (1,)), ((), ())), preferred_element_type=jnp.float32
    )
    deriv = packed_ref[:slots, width + wide : width + wide + units].astype(jnp.float32)
    pg_ref[...] = jnp.zeros_like(pg_ref)
    pg_ref[:, :units] = (hidden_grad * deriv).astype(jnp.bfloat16)
    near, _, block, _ = mine_ref.shape
    keep = wide - LANE
    step = width // 2
    low = lax.axis_index("dp") % 2 == 0
    hidden = packed_ref[:slots, width : width + wide]
    for at in range(0, width, step):
        dims = (((0,), (0,)), ((), ()))
        first = lax.dot_general(packed_ref[:slots, at : at + step], pg_ref[...], dims, preferred_element_type=jnp.float32)
        second = lax.dot_general(up_ref[:, at : at + step], hidden, dims, preferred_element_type=jnp.float32)
        for b in range(0, step, 2 * block):
            m, p = divmod((at + b) // (2 * block), near)
            parts = []
            for half in (b, b + block):
                one, two = first[half : half + block] * factor, second[half : half + block] * factor
                parts.append((one[:, :keep], one[:, keep:] + two[:, :LANE], two[:, LANE:]))
            for lo, hi, start in zip(*parts, (0, keep, wide)):
                mine_ref[p, m, :, start : start + lo.shape[1]] = jnp.where(low, lo, hi).astype(jnp.bfloat16)
                theirs_ref[p, m, :, start : start + lo.shape[1]] = jnp.where(low, hi, lo).astype(jnp.bfloat16)


def grad_terms(tiles, packed, units, width, rows, factor, shape):
    slots = tiles.shape[0] * SLOT_PAD
    wide = -(-units // LANE) * LANE
    _, places = tile_places(rows, width, tiles.shape[0])
    return pl.pallas_call(
        functools.partial(grads_kernel, places, factor, units),
        out_shape=(jax.ShapeDtypeStruct(shape, jnp.bfloat16),) * 2,
        scratch_shapes=[
            pltpu.VMEM((rows, width), jnp.bfloat16),
            pltpu.VMEM((slots, width), jnp.bfloat16),
            pltpu.VMEM((slots, wide), jnp.bfloat16),
        ],
        name="grad_terms",
        compiler_params=pltpu.CompilerParams(vmem_limit_bytes=GRADS_VMEM << 20),
    )(tiles, packed)


def tables_kernel(side, ranks_ref, table_ref, early_ref):
    rows = ranks_ref.shape[1]
    slots = table_ref.shape[0]
    groups = slots // SLOT_PAD
    ranks = ranks_ref[...]
    hot = lax.broadcasted_iota(jnp.int32, (groups, rows), 0) == ranks
    earlier = lax.broadcasted_iota(jnp.int32, (rows, rows), 0) < lax.broadcasted_iota(jnp.int32, (rows, rows), 1)
    before = jnp.dot(
        hot.astype(jnp.float32).astype(jnp.bfloat16),
        earlier.astype(jnp.float32).astype(jnp.bfloat16),
        preferred_element_type=jnp.float32,
    )
    position = jnp.sum(jnp.where(hot, before, 0.0), axis=0, keepdims=True).astype(jnp.int32)
    targets = lax.broadcasted_iota(jnp.int32, (slots, rows), 0)
    table_ref[...] = (targets == ranks * SLOT_PAD + position).astype(jnp.float32).astype(jnp.bfloat16)
    shift = side.bit_length() - 1
    me = lax.axis_index("tp")
    dx = ((ranks >> shift) - (me >> shift)) & (side - 1)
    dy = ((ranks & (side - 1)) - (me & (side - 1))) & (side - 1)
    x_first = lax.axis_index("dp") % 2 == 0
    where_to = jnp.where(x_first, dx * side + dy, dy * side + dx)
    early_ref[...] = (targets == where_to * SLOT_PAD + position).astype(jnp.float32).astype(jnp.bfloat16)


def slot_tables(rank_ids, groups):
    shape = jax.ShapeDtypeStruct((groups * SLOT_PAD, rank_ids.shape[1]), jnp.bfloat16)
    return pl.pallas_call(
        functools.partial(tables_kernel, int(groups**0.5)), out_shape=(shape, shape), name="slot_tables",
    )(rank_ids)


def exchange(blocks, axis, groups=None):
    return lax.all_to_all(blocks, axis, 0, 0, tiled=True, axis_index_groups=groups)


def to_all(shard, axis):
    return exchange(jnp.broadcast_to(shard, (lax.axis_size(axis), *shard.shape)), axis)


def total(arrived):
    return arrived.astype(jnp.float32).sum(axis=0).astype(jnp.bfloat16)


def plane_rounds(replicas, side):
    rounds = []
    for turn in range(2):
        perms = []
        for d in range(1, side):
            pairs = []
            for k in range(replicas):
                for x in range(side):
                    for y in range(side):
                        along_x = (k % 2 == 0) == (turn == 0)
                        to = ((x + d) % side, y) if along_x else (x, (y + d) % side)
                        pairs.append(((k * side + x) * side + y, (k * side + to[0]) * side + to[1]))
            perms.append(pairs)
        rounds.append(perms)
    return rounds


def named_permute(value, pairs):
    return lax.ppermute(value, ("dp", "tp"), pairs)


def summed(own, moved):
    return sum((b.astype(jnp.float32) for b in moved), own.astype(jnp.float32)).astype(jnp.bfloat16)


def route_early(part, table, replicas, groups):
    side = int(groups**0.5)
    rounds = plane_rounds(replicas, side)
    span = side * SLOT_PAD
    blocks = []
    for d in range(side):
        block = jnp.dot(table[d * span : (d + 1) * span], part, preferred_element_type=jnp.float32)
        blocks.append(block.astype(jnp.bfloat16))
    moved = [named_permute(blocks[d], rounds[0][d - 1]) for d in range(1, side)]
    half_way = summed(lax.optimization_barrier(blocks[0]), moved)
    pieces = [half_way[d * SLOT_PAD : (d + 1) * SLOT_PAD] for d in range(side)]
    moved = [named_permute(pieces[d], rounds[1][d - 1]) for d in range(1, side)]
    return summed(pieces[0], moved)


def dp_groups(replicas):
    cores, near = 2, 4
    depth = replicas // cores
    far = depth // near
    pairs = [(k, k ^ 1) for k in range(replicas)]
    close = []
    for g in range(far):
        close.append([cores * (near * g + p) for p in range(near)])
    for g in range(far):
        zs = [(near * (g + 1) + p) % depth if p < near // 2 else near * g + p for p in range(near)]
        close.append([cores * z + 1 for z in zs])
    strided = [[cores * (near * m + p) + c for m in range(far)] for p in range(near) for c in range(cores)]
    return cores, near, far, pairs, close, strided


def shards(partials, layer_input, ln_gain, ln_bias, fc1_weight, fc1_bias, fc2_weight, row_rank):
    groups = lax.axis_size("tp")
    replicas = lax.axis_size("dp")
    local_part = partials[0]
    row_count = local_part.shape[0]
    slot_count, width = layer_input.shape
    units = fc1_weight.shape[1]
    _, near, far, pairs, close, strided = dp_groups(replicas)
    block = width // replicas

    arrived = exchange(cut_tiles(local_part, layer_input, groups), "tp")
    head = arrived.shape[1] - (SLOT_PAD // SUB) * (width // LANE)
    own_tiles = total(arrived[:, :head])
    tiles = to_all(own_tiles, "tp")

    table, early_table = slot_tables(row_rank.T, groups)
    packed = hidden_parts(arrived, head, ln_gain, ln_bias, fc1_weight.T, fc1_bias, table, fc2_weight.T)
    placed = route_early(local_part[:, width:], early_table, replicas, groups)[:slot_count]

    factor = float(replicas * row_count) ** (-0.5)
    mine, theirs = grad_terms(
        tiles, packed, units, width, row_count, factor,
        (near, far, block, 2 * units),
    )
    theirs = lax.ppermute(theirs, "dp", pairs)
    both = summed(mine, (theirs,))
    both = exchange(both, "dp", close)
    both = total(both)
    both = exchange(both, "dp", strided)
    both = total(both)
    first, second = both[:, :units], both[:, units:]
    return (placed, first, second)


def solution(mesh):
    return jax.shard_map(
        shards,
        mesh=mesh,
        in_specs=(
            P("tp", "dp", None),
            P(("dp", "tp"), None),
            P(),
            P(),
            P(None, "tp"),
            P("tp"),
            P(None, "tp"),
            P("dp", None),
        ),
        out_specs=(P(("dp", "tp"), None), P("dp", "tp"), P("dp", "tp")),
        check_vma=False,
    )
```
